256 devices in a mesh: img: 2 (over z), ga: 16 (over y, core), band: 8 (over x).
Axes of the slice: x: 8, y: 8, z: 2, core: 2. Of those that a mesh axis runs over, the one named last changes fastest.
The devices are a block of a 8x8x16 slice.
Arguments:
- orbitals: bfloat16 [1536, 49152], P(('img', 'band'), 'ga'), parts along dimension 0, as said below
- kernel: float32 [49152], P('ga'), may hold values from 0.3 to 3
- block_vectors: bfloat16 [512, 49152], P(('img', 'band'), 'ga'), parts along dimension 0
Outputs:
- ace_vectors: bfloat16 [1536, 49152], P(('img', 'band'), 'ga'), parts along dimension 0
- exchange_block: bfloat16 [512, 49152], P(('img', 'band'), 'ga'), parts along dimension 0
The draws below stay inside these ranges and needn't reach their ends.
There are 2 independent parts, one for each index of `img`. The reference program is written for one: setup_inputs(seed, part) draws one part's arguments, and reference() takes and returns one part's arrays. A program takes and returns all parts, laid end to end along the dimension named above; an argument that names none is the same for every part. Nothing has to cross between parts.
Inputs may be any that keep to these rules, and one draw needn't show every extreme that they name: `orbitals`: the bands of one image are linearly independent, and the block lies largely in their span.
All inputs are finite; a program needn't handle non-finite values.
Results may differ from the reference program's by a relative error of at most 0.02.
Values may be sent and summed in bfloat16 or wider, within the bound.
A program may use at most 64 MiB of HBM per device.

```python
import math
import jax
import jax.numpy as jnp
from jax import lax

NB = 768
NBLK = 256
NG = 49152


def orbital_pair(key):
    independent = jax.random.normal(jax.random.fold_in(key, 11), (NB, NG), jnp.float32)
    mixing = jax.random.normal(jax.random.fold_in(key, 12), (NB, NB), jnp.float32) * (0.4 / math.sqrt(NB))
    orbital_rows = independent + jnp.dot(mixing, independent, precision=lax.Precision.HIGHEST)
    mixture = jax.random.normal(jax.random.fold_in(key, 13), (NBLK, NB), jnp.float32) / math.sqrt(NB)
    residue = jax.random.normal(jax.random.fold_in(key, 14), (NBLK, NG), jnp.float32)
    block_rows = jnp.dot(mixture, orbital_rows, precision=lax.Precision.HIGHEST) + 0.5 * residue
    return (orbital_rows, block_rows)


def draw_orbitals(key, part):
    return orbital_pair(key)[0].astype(jnp.bfloat16)


def draw_block_vectors(key, part):
    return orbital_pair(key)[1].astype(jnp.bfloat16)


def steps_of(rng, extent, pieces, least, high):
    gain, own = 1.0, jax.random.fold_in(rng, 6)
    for position, blocks in pieces:
        heights = jnp.exp(jax.random.uniform(jax.random.fold_in(own, position), (blocks,), jnp.float32, least / len(pieces), high / len(pieces)))
        gain = gain * jnp.repeat(heights, extent[position] // blocks).reshape([-1 if axis == position else 1 for axis in range(len(extent))])
    return gain


def setup_inputs(seed: int = 0, part: int = 0) -> dict:
    arg_keys = jax.random.split(jax.random.key(seed), 4)
    part_keys = jax.random.split(jax.random.fold_in(arg_keys[3], part), 4)
    orbitals = draw_orbitals(jax.random.fold_in(jax.random.fold_in(arg_keys[3], part), 71), part)
    kernel = jnp.clip(jnp.exp(math.log(3.0) - 2.3025851 * jax.random.uniform(arg_keys[1], (NG,), jnp.float32) ** steps_of(arg_keys[1], (NG,), ((0, 16),), -0.2, 0.2)), 0.3, 3.0)
    block_vectors = draw_block_vectors(jax.random.fold_in(jax.random.fold_in(arg_keys[3], part), 71), part)
    return {"orbitals": orbitals, "kernel": kernel, "block_vectors": block_vectors}


def reference(orbitals, kernel, block_vectors):
    weighted = (-(orbitals.astype(jnp.float32) * kernel[None, :])).astype(jnp.bfloat16)
    margin = -lax.dot_general(orbitals.astype(jnp.float32), weighted.astype(jnp.float32), (((1,), (1,)), ((), ())), preferred_element_type=jnp.float32) / NG
    factor = jnp.linalg.cholesky(margin)
    projector = lax.linalg.triangular_solve(factor, weighted.astype(jnp.float32), left_side=True, lower=True)
    coupling = jnp.dot(projector, block_vectors.astype(jnp.float32).T, precision=lax.Precision.HIGHEST) / NG
    applied = -lax.dot_general(coupling, projector, (((0,), (0,)), ((), ())), precision=lax.Precision.HIGHEST)
    return (projector.astype(jnp.bfloat16), applied.astype(jnp.bfloat16))
```

```python
import functools
import jax
import jax.numpy as jnp
from jax import lax
from jax.experimental import pallas as pl
from jax.experimental.pallas import tpu as pltpu
from jax.sharding import PartitionSpec as P

LANES = 128
SUB = 8
TILE = 128
CORES = 2
MESH = pl.DeviceIdType.MESH
F32 = jnp.float32
BF16 = jnp.bfloat16
VMEM = pl.BlockSpec(memory_space=pltpu.VMEM)


def row_of(value, index):
    return jnp.broadcast_to(value[index : index + 1, :], value.shape)


def column_of(value, index):
    return jnp.broadcast_to(value[:, index : index + 1], value.shape)


def inverse_factor(rows):
    sub = lax.broadcasted_iota(jnp.int32, (SUB, LANES), 0)
    lane = lax.broadcasted_iota(jnp.int32, (SUB, LANES), 1)
    rows = list(rows)
    count = len(rows)
    done = []
    for t in range(count):
        first = t * SUB
        inside = (lane >= first) & (lane < first + SUB)
        strip = rows[t]
        columns = [column_of(strip, first + k) for k in range(SUB)]
        strip = jnp.where(inside, jnp.where(lane - first == sub, 1.0, 0.0), strip)
        forward = strip
        scale = jnp.ones((SUB, LANES), F32)
        for j in range(SUB):
            pivot = 1.0 / row_of(columns[j], j)
            scale = jnp.where(sub == j, pivot, scale)
            factor = jnp.where(sub == j, 0.0, columns[j] * pivot)
            for k in range(j + 1, SUB):
                columns[k] = columns[k] - factor * row_of(columns[k], j)
            strip = strip - factor * row_of(strip, j)
            if j < SUB - 1:
                forward = forward - jnp.where(sub > j, factor, 0.0) * row_of(forward, j)
        done.append(jnp.where(lane < first + SUB, forward * jnp.sqrt(scale), 0.0))
        if t == count - 1:
            break
        solved = strip * scale
        solved_rows = [row_of(solved, j) for j in range(SUB)]
        for r in range(t + 1, count):
            old = rows[r]
            total = jnp.where(inside, 0.0, old)
            terms = [column_of(old, first + j) * solved_rows[j] for j in range(SUB)]
            while len(terms) > 1:
                terms = [terms[i] + terms[i + 1] for i in range(0, len(terms), 2)]
            rows[r] = total - terms[0]
    return done


def split(value):
    high = value.astype(BF16)
    return high, (value - high.astype(F32)).astype(BF16)


def dot(left, right):
    return lax.dot_general(left, right, (((1,), (0,)), ((), ())), preferred_element_type=F32)


def dot_rows(left, right):
    return lax.dot_general(left, right, (((1,), (1,)), ((), ())), preferred_element_type=F32)


def dot_split(left, right):
    (lh, ll), (rh, rl) = left, right
    return dot(lh, rh) + dot(lh, rl) + dot(ll, rh)


def blocks_of(bands, vectors):
    tiles = bands // TILE
    margin = [(i, j) for i in range(tiles) for j in range(i, tiles)]
    overlap = [(i, j) for i in range(tiles) for j in range(vectors // TILE)]
    where_margin = {ij: n * TILE for n, ij in enumerate(margin)}
    where_overlap = {ij: (len(margin) + n) * TILE for n, ij in enumerate(overlap)}
    return where_margin, where_overlap, (len(margin) + len(overlap)) * TILE


def solve_kernel(bands, vectors, packed_ref, weighted_ref, ace_ref, exchange_ref, work):
    width = weighted_ref.shape[1]
    tiles = bands // TILE
    where_margin, where_overlap, _ = blocks_of(bands, vectors)
    for (i, j), row in where_margin.items():
        work[pl.ds(i * TILE, TILE), pl.ds(j * TILE, TILE)] = packed_ref[pl.ds(row, TILE), :].astype(F32)
    for (i, j), row in where_overlap.items():
        work[pl.ds(i * TILE, TILE), pl.ds(bands + j * TILE, TILE)] = packed_ref[
            pl.ds(row, TILE), :
        ].astype(F32)
    for i in range(tiles):
        work[pl.ds(i * TILE, TILE), pl.ds(bands + vectors, width)] = weighted_ref[
            pl.ds(i * TILE, TILE), :
        ].astype(F32)
    applied = None
    for k in range(tiles):
        top = k * TILE
        strips = [work[pl.ds(top + SUB * t, SUB), pl.ds(top, TILE)] for t in range(TILE // SUB)]
        inverse = jnp.concatenate(inverse_factor(strips), axis=0)
        first = top + TILE
        rest = work[pl.ds(top, TILE), pl.ds(first, work.shape[1] - first)]
        upper = dot_split(split(inverse), split(rest))
        parts = split(upper)
        for i in range(k + 1, tiles):
            at = i * TILE - first
            lower = split(upper[:, at : at + TILE].T)
            cut = tuple(part[:, at:] for part in parts)
            rows = pl.ds(i * TILE, TILE)
            cols = pl.ds(i * TILE, work.shape[1] - i * TILE)
            work[rows, cols] = work[rows, cols] - dot_split(lower, cut)
        base = bands - first
        coupling = split(upper[:, base : base + vectors].T)
        projector = tuple(part[:, base + vectors :] for part in parts)
        ace_ref[pl.ds(top, TILE), :] = upper[:, base + vectors :].astype(BF16)
        term = dot_split(coupling, projector)
        applied = term if applied is None else applied + term
    exchange_ref[...] = (-applied).astype(BF16)


def solve(packed, weighted, bands, vectors):
    width = weighted.shape[1]
    return pl.pallas_call(
        functools.partial(solve_kernel, bands, vectors),
        out_shape=(
            jax.ShapeDtypeStruct((bands, width), BF16),
            jax.ShapeDtypeStruct((vectors, width), BF16),
        ),
        in_specs=[VMEM, VMEM],
        out_specs=(VMEM, VMEM),
        scratch_shapes=[pltpu.VMEM((bands, bands + vectors + width), F32)],
        compiler_params=pltpu.CompilerParams(vmem_limit_bytes=40 * 2**20),
        name="solve",
    )(packed, weighted)


def remote(src, dst, send, recv, band, ga):
    return pltpu.make_async_remote_copy(
        src_ref=src,
        dst_ref=dst,
        send_sem=send,
        recv_sem=recv,
        device_id={"band": band, "ga": ga},
        device_id_type=MESH,
    )


def meet(devices):
    barrier = pltpu.get_barrier_semaphore()
    for band, ga in devices:
        pl.semaphore_signal(barrier, inc=1, device_id={"band": band, "ga": ga}, device_id_type=MESH)
    pl.semaphore_wait(barrier, len(devices))


def aligned(start, step, size):
    return pl.ds(pl.multiple_of(start, step), size)


def front_kernel(
    count, groups, total, orbitals_ref, block_ref, kernel_ref, packed_ref, weighted_ref,
    bands, vectors, part, half_in, half, first_in, own, second_in,
    to_bands, from_bands, to_vectors, from_vectors, pair_send, pair_recv,
    first_send, first_recv, second_send, second_recv,
    spread_send, spread_recv, give_send, give_recv,
):
    band, ga = lax.axis_index("band"), lax.axis_index("ga")
    line, core = ga // CORES, ga % CORES
    rows, cols = orbitals_ref.shape[0], weighted_ref.shape[1]
    block_rows = block_ref.shape[0]
    here = (1 - core) * band + core * line
    there = (1 - core) * line + core * band

    def along_first(q):
        return (1 - core) * q + core * band, CORES * ((1 - core) * line + core * q) + core

    def along_second(q):
        return (1 - core) * band + core * q, CORES * ((1 - core) * q + core * line) + core

    pair = (band, CORES * line + 1 - core)
    steps = range(1, count)
    meet(
        [along_first((here + d) % count) for d in steps]
        + [along_second((there + d) % count) for d in steps]
        + [pair]
    )

    moved = []
    for d in steps:
        peer = (band + d) % count
        mine = aligned(peer * cols, LANES, cols)
        moved.append((
            remote(orbitals_ref.at[:, mine], bands.at[aligned(band * rows, 16, rows), :],
                   to_bands.at[d - 1], from_bands.at[d - 1], peer, ga),
            remote(block_ref.at[:, mine], vectors.at[aligned(band * block_rows, 16, block_rows), :],
                   to_vectors.at[d - 1], from_vectors.at[d - 1], peer, ga),
        ))
    for orbital_copy, _ in moved:
        orbital_copy.start()
    for _, block_copy in moved:
        block_copy.start()
    mine = aligned(band * cols, LANES, cols)
    bands[aligned(band * rows, 16, rows), :] = orbitals_ref[:, mine]
    vectors[aligned(band * block_rows, 16, block_rows), :] = block_ref[:, mine]
    gains = kernel_ref[:, mine]
    for orbital_copy, _ in moved:
        orbital_copy.wait()

    all_rows, all_vectors = bands.shape[0], vectors.shape[0]
    tiles = all_rows // TILE
    where_margin, where_overlap, used = blocks_of(all_rows, all_vectors)
    for i in range(tiles):
        at = pl.ds(i * TILE, TILE)
        weighted_ref[at, :] = (-(bands[at, :].astype(F32) * gains)).astype(BF16)
    for i in range(tiles):
        at, after = pl.ds(i * TILE, TILE), pl.ds(i * TILE, all_rows - i * TILE)
        sums = dot_rows(bands[at, :], weighted_ref[after, :]) + dot_rows(weighted_ref[at, :], bands[after, :])
        sums = (sums * (-0.5 / total)).astype(BF16)
        for j in range(i, tiles):
            part[pl.ds(where_margin[i, j], TILE), :] = sums[:, (j - i) * TILE : (j - i + 1) * TILE]
    for _, block_copy in moved:
        block_copy.wait()
    for i in range(tiles):
        sums = dot_rows(weighted_ref[pl.ds(i * TILE, TILE), :], vectors[...])
        sums = (sums * (1.0 / total)).astype(BF16)
        for j in range(all_vectors // TILE):
            part[pl.ds(where_overlap[i, j], TILE), :] = sums[:, j * TILE : (j + 1) * TILE]
    if used < part.shape[0]:
        part[used:, :] = jnp.zeros((part.shape[0] - used, LANES), BF16)

    piece = part.shape[0] // (CORES * count)
    size = piece * count

    def piece_at(core_of, q):
        return aligned((core_of * count + q) * piece, 16, piece)

    swap = remote(part.at[aligned((1 - core) * size, 16, size), :], half_in, pair_send, pair_recv, *pair)
    swap.start()
    swap.wait()

    first = []
    for d in range(1, count + 1):
        q = (here + d) % count
        there_in = half_in[aligned(q * piece, 16, piece), :].astype(F32)
        summed = (part[piece_at(core, q), :].astype(F32) + there_in).astype(BF16)
        if d < count:
            half[d - 1] = summed
            copy = remote(half.at[d - 1], first_in.at[d - 1], first_send.at[d - 1], first_recv.at[d - 1],
                          *along_first(q))
            copy.start()
            first.append(copy)
    summed = summed.astype(F32)
    for d, copy in enumerate(first):
        copy.wait()
        summed = summed + first_in[d].astype(F32)
    own[...] = summed.astype(BF16)

    second = []
    for d in steps:
        copy = remote(own, second_in.at[there], second_send.at[d - 1], second_recv.at[d - 1],
                      *along_second((there + d) % count))
        copy.start()
        second.append(copy)
    second_in[there] = own[...]
    for copy in second:
        copy.wait()
    summed = second_in[0].astype(F32)
    for q in steps:
        summed = summed + second_in[q].astype(F32)
    place = piece_at(core, here)
    packed_ref[place, :] = summed.astype(BF16)

    give = []

    def pass_on(slot, q):
        at = packed_ref.at[piece_at(core, q), :]
        copy = remote(at, at, give_send.at[slot], give_recv.at[slot], *pair)
        copy.start()
        give.append(copy)

    spread = []
    for d in steps:
        at = packed_ref.at[place, :]
        copy = remote(at, at, spread_send.at[d - 1], spread_recv.at[d - 1], *along_first((here + d) % count))
        copy.start()
        spread.append(copy)
    pass_on(0, here)
    for d in steps:
        spread[d - 1].wait_recv()
        pass_on(d, (here - d + count) % count)
    for copy in spread:
        copy.wait_send()
    for copy in give:
        copy.wait()


def front(orbitals, block_vectors, kernel, count, groups):
    rows, coeffs = orbitals.shape
    block_rows = block_vectors.shape[0]
    bands, vectors, cols = rows * count, block_rows * count, coeffs // count
    _, _, used = blocks_of(bands, vectors)
    pieces = CORES * count
    piece = pl.cdiv(pl.cdiv(used, pieces), 16) * 16
    sems = pltpu.SemaphoreType.DMA
    seven = sems((count - 1,))
    return pl.pallas_call(
        functools.partial(front_kernel, count, groups, coeffs * groups),
        out_shape=(
            jax.ShapeDtypeStruct((pieces * piece, LANES), BF16),
            jax.ShapeDtypeStruct((bands, cols), BF16),
        ),
        in_specs=[VMEM, VMEM, VMEM],
        out_specs=(VMEM, VMEM),
        scratch_shapes=[
            pltpu.VMEM((bands, cols), BF16),
            pltpu.VMEM((vectors, cols), BF16),
            pltpu.VMEM((pieces * piece, LANES), BF16),
            pltpu.VMEM((count * piece, LANES), BF16),
            pltpu.VMEM((count - 1, piece, LANES), BF16),
            pltpu.VMEM((count - 1, piece, LANES), BF16),
            pltpu.VMEM((piece, LANES), BF16),
            pltpu.VMEM((count, piece, LANES), BF16),
            seven, seven, seven, seven, sems, sems,
            seven, seven, seven, seven, seven, seven, sems((count,)), sems((count,)),
        ],
        compiler_params=pltpu.CompilerParams(
            collective_id=0, has_side_effects=True, vmem_limit_bytes=40 * 2**20
        ),
        name="front",
    )(orbitals, block_vectors, kernel[None, :])


def back_kernel(
    count, ace_ref, exchange_ref, ace_out, exchange_out, to_ace, from_ace, to_block, from_block
):
    band, ga = lax.axis_index("band"), lax.axis_index("ga")
    rows, cols = ace_out.shape[0], ace_ref.shape[1]
    block_rows = exchange_out.shape[0]
    steps = range(1, count)
    meet([((band + d) % count, ga) for d in steps])
    place = aligned(band * cols, LANES, cols)
    copies = []
    for d in steps:
        peer = (band + d) % count
        copies.append(
            remote(ace_ref.at[aligned(peer * rows, 16, rows), :], ace_out.at[:, place],
                   to_ace.at[d - 1], from_ace.at[d - 1], peer, ga)
        )
        copies.append(
            remote(exchange_ref.at[aligned(peer * block_rows, 16, block_rows), :], exchange_out.at[:, place],
                   to_block.at[d - 1], from_block.at[d - 1], peer, ga)
        )
    for copy in copies:
        copy.start()
    ace_out[:, place] = ace_ref[aligned(band * rows, 16, rows), :]
    exchange_out[:, place] = exchange_ref[aligned(band * block_rows, 16, block_rows), :]
    for copy in copies:
        copy.wait()


def back(ace, exchange, count):
    bands, cols = ace.shape
    vectors = exchange.shape[0]
    seven = pltpu.SemaphoreType.DMA((count - 1,))
    return pl.pallas_call(
        functools.partial(back_kernel, count),
        out_shape=(
            jax.ShapeDtypeStruct((bands // count, cols * count), BF16),
            jax.ShapeDtypeStruct((vectors // count, cols * count), BF16),
        ),
        in_specs=[VMEM, VMEM],
        out_specs=(VMEM, VMEM),
        scratch_shapes=[seven, seven, seven, seven],
        compiler_params=pltpu.CompilerParams(
            collective_id=1, has_side_effects=True, vmem_limit_bytes=20 * 2**20
        ),
        name="back",
    )(ace, exchange)


def shards(count, groups, orbitals, kernel, block_vectors):
    packed, weighted = front(orbitals, block_vectors, kernel, count, groups)
    ace, exchange = solve(packed, weighted, orbitals.shape[0] * count, block_vectors.shape[0] * count)
    return back(ace, exchange, count)


def solution(mesh):
    placed = (P(("img", "band"), "ga"), P("ga"), P(("img", "band"), "ga"))
    return jax.shard_map(
        functools.partial(shards, mesh.shape["band"], mesh.shape["ga"]),
        mesh=mesh,
        in_specs=placed,
        out_specs=(P(("img", "band"), "ga"), P(("img", "band"), "ga")),
        check_vma=False,
    )
```

```python
import functools
import jax
import jax.numpy as jnp
from jax import lax
from jax.experimental import pallas as pl
from jax.experimental.pallas import tpu as pltpu
from jax.sharding import PartitionSpec as P

LANES = 128
SUB = 8
TILE = 128
PANEL = 32
GROUP = 2
CORES = 2
MESH = pl.DeviceIdType.MESH
F32 = jnp.float32
BF16 = jnp.bfloat16
VMEM = pl.BlockSpec(memory_space=pltpu.VMEM)


def row_of(value, index):
    return jnp.broadcast_to(value[index : index + 1, :], value.shape)


def column_of(value, index):
    return jnp.take_along_axis(value, jnp.full(value.shape, index, jnp.int32), axis=1)


def inverse_factor(rows):
    sub = lax.broadcasted_iota(jnp.int32, (SUB, LANES), 0)
    lane = lax.broadcasted_iota(jnp.int32, (SUB, LANES), 1)
    rows = list(rows)
    count = len(rows)
    per_panel = PANEL // SUB
    size = GROUP * SUB
    done = []
    for begin in range(0, count, GROUP):
        first = begin * SUB
        last = (begin // per_panel + 1) * per_panel
        inside = (lane >= first) & (lane < first + size)
        strips = rows[begin : begin + GROUP]
        columns = [[column_of(strip, first + k) for k in range(size)] for strip in strips]
        solved = [
            jnp.where(inside, jnp.where(lane - first == sub + s * SUB, 1.0, 0.0), strips[s])
            for s in range(GROUP)
        ]
        forward = list(solved)
        scale = [jnp.ones((SUB, LANES), F32)] * GROUP
        diagonal = [jnp.ones((SUB, LANES), F32)] * GROUP
        for j in range(size):
            js, jj = divmod(j, SUB)
            value = row_of(columns[js][j], jj)
            pivot = 1.0 / value
            here = sub == jj
            scale[js] = jnp.where(here, pivot, scale[js])
            diagonal[js] = jnp.where(here, value, diagonal[js])
            factor = [columns[s][j] * pivot for s in range(GROUP)]
            factor[js] = jnp.where(here, 0.0, factor[js])
            for k in range(j + 1, size):
                row = row_of(columns[js][k], jj)
                for s in range(GROUP):
                    columns[s][k] = columns[s][k] - factor[s] * row
            row = row_of(forward[js], jj)
            if jj < SUB - 1:
                forward[js] = forward[js] - jnp.where(sub > jj, factor[js], 0.0) * row
            for s in range(js + 1, GROUP):
                forward[s] = forward[s] - factor[s] * row
            row = row_of(solved[js], jj)
            for s in range(GROUP):
                solved[s] = solved[s] - factor[s] * row
        for s in range(GROUP):
            kept = forward[s] * lax.rsqrt(diagonal[s])
            stop = first + (s + 1) * SUB
            if stop < last * SUB:
                kept = jnp.where((lane < stop) | (lane >= last * SUB), kept, 0.0)
            done.append(kept)
        after = begin + GROUP
        if after < last:
            solved_rows = [row_of(solved[s] * scale[s], jj) for s in range(GROUP) for jj in range(SUB)]
            for r in range(after, last):
                old = rows[r]
                total = jnp.where(inside, 0.0, old)
                terms = [column_of(old, first + j) * solved_rows[j] for j in range(size)]
                while len(terms) > 1:
                    terms = [terms[i] + terms[i + 1] for i in range(0, len(terms), 2)]
                rows[r] = total - terms[0]
        elif last < count:
            start = last - per_panel
            upper = jnp.concatenate(done[start:last], axis=0)
            product = dot_split(split(upper.T), split(upper))
            gone = (lane >= start * SUB) & (lane < last * SUB)
            for r in range(last, count):
                rows[r] = jnp.where(gone, 0.0, rows[r]) - product[r * SUB : r * SUB + SUB, :]
    return [jnp.where(lane < (t + 1) * SUB, done[t], 0.0) for t in range(count)]


def split(value):
    high = value.astype(BF16)
    return high, (value - high.astype(F32)).astype(BF16)


def dot(left, right):
    return lax.dot_general(left, right, (((1,), (0,)), ((), ())), preferred_element_type=F32)


def dot_rows(left, right):
    return lax.dot_general(left, right, (((1,), (1,)), ((), ())), preferred_element_type=F32)


def dot_split(left, right):
    (lh, ll), (rh, rl) = left, right
    return dot(lh, rh) + dot(lh, rl) + dot(ll, rh)


def remote(src, dst, send, recv, band, ga):
    return pltpu.make_async_remote_copy(
        src_ref=src,
        dst_ref=dst,
        send_sem=send,
        recv_sem=recv,
        device_id={"band": band, "ga": ga},
        device_id_type=MESH,
    )


def meet(devices):
    barrier = pltpu.get_barrier_semaphore()
    for band, ga in devices:
        pl.semaphore_signal(barrier, inc=1, device_id={"band": band, "ga": ga}, device_id_type=MESH)
    pl.semaphore_wait(barrier, len(devices))


def aligned(start, step, size):
    return pl.ds(pl.multiple_of(start, step), size)


def ring(position, count):
    return [(position + d) % count for d in range(1, count)]


def all_reduce(count, place, part, half_in, half, first_in, own, second_in, out, send, recv):
    core, here, there, along_first, along_second, pair = place
    piece = part.shape[0] // (CORES * count)
    size = piece * count
    pair_at, first_at, second_at, spread_at, give_at = 0, 1, count, 2 * count - 1, 3 * count - 2
    steps = range(1, count)

    def piece_at(q):
        return aligned((core * count + q) * piece, 16, piece)

    def copy_to(src, dst, sem, device):
        copy = remote(src, dst, send.at[sem], recv.at[sem], *device)
        copy.start()
        return copy

    swap = copy_to(part.at[aligned((1 - core) * size, 16, size), :], half_in, pair_at, pair)
    yield
    swap.wait()
    copies = []
    for d in range(1, count + 1):
        q = (here + d) % count
        theirs = half_in[aligned(q * piece, 16, piece), :].astype(F32)
        summed = part[piece_at(q), :].astype(F32) + theirs
        if d < count:
            half[d - 1] = summed.astype(BF16)
            copies.append(copy_to(half.at[d - 1], first_in.at[d - 1], first_at + d - 1, along_first(q)))
    yield
    for d, copy in enumerate(copies):
        copy.wait()
        summed = summed + first_in[d].astype(F32)
    own[...] = summed.astype(BF16)
    copies = []
    for d in steps:
        device = along_second((there + d) % count)
        copies.append(copy_to(own, second_in.at[there], second_at + d - 1, device))
    second_in[there] = own[...]
    yield
    for copy in copies:
        copy.wait()
    summed = second_in[0].astype(F32)
    for q in steps:
        summed = summed + second_in[q].astype(F32)
    out[piece_at(here), :] = summed.astype(BF16)
    copies, given = [], []

    def pass_on(slot, q):
        at = out.at[piece_at(q), :]
        given.append(copy_to(at, at, give_at + slot, pair))

    for d in steps:
        at = out.at[piece_at(here), :]
        copies.append(copy_to(at, at, spread_at + d - 1, along_first((here + d) % count)))
    pass_on(0, here)
    yield
    for d in steps:
        copies[d - 1].wait_recv()
        pass_on(d, (here - d + count) % count)
    yield
    for copy in copies:
        copy.wait_send()
    for copy in given:
        copy.wait()
    yield


def ace_kernel(
    count, groups, orbitals_ref, block_ref, kernel_ref, ace_out, exchange_out,
    orbitals, block, gains, bands, vectors, weighted, work, ace, exchange,
    margin_part, margin_half_in, margin_half, margin_first, margin_own, margin_second, margin,
    overlap_part, overlap_half_in, overlap_half, overlap_first, overlap_own, overlap_second, overlap,
    load, to_bands, from_bands, to_vectors, from_vectors, margin_send, margin_recv, overlap_send, overlap_recv,
    to_ace, from_ace, to_block, from_block,
):
    band, ga = lax.axis_index("band"), lax.axis_index("ga")
    line, core = ga // CORES, ga % CORES
    rows, cols = orbitals.shape[0], weighted.shape[1]
    block_rows = block.shape[0]
    total = orbitals.shape[1] * groups
    here = (1 - core) * band + core * line
    there = (1 - core) * line + core * band

    def along_first(q):
        return (1 - core) * q + core * band, CORES * ((1 - core) * line + core * q) + core

    def along_second(q):
        return (1 - core) * band + core * q, CORES * ((1 - core) * q + core * line) + core

    pair = (band, CORES * line + 1 - core)
    place = (core, here, there, along_first, along_second, pair)

    loads = [
        pltpu.make_async_copy(orbitals_ref, orbitals, load.at[0]),
        pltpu.make_async_copy(block_ref, block, load.at[1]),
        pltpu.make_async_copy(kernel_ref, gains, load.at[2]),
    ]
    for copy in loads:
        copy.start()
    meet(
        [along_first(q) for q in ring(here, count)]
        + [along_second(q) for q in ring(there, count)]
        + [pair]
    )
    for copy in loads:
        copy.wait()

    mine = aligned(band * cols, LANES, cols)
    band_rows = aligned(band * rows, 16, rows)
    vector_rows = aligned(band * block_rows, 16, block_rows)
    moved, moved_block = [], []
    for d, peer in enumerate(ring(band, count)):
        theirs = aligned(peer * cols, LANES, cols)
        moved.append(
            remote(orbitals.at[:, theirs], bands.at[band_rows, :], to_bands.at[d], from_bands.at[d], peer, ga)
        )
        moved_block.append(
            remote(block.at[:, theirs], vectors.at[vector_rows, :], to_vectors.at[d], from_vectors.at[d], peer, ga)
        )
    for copy in moved + moved_block:
        copy.start()
    bands[band_rows, :] = orbitals[:, mine]
    vectors[vector_rows, :] = block[:, mine]
    gain = gains[:, mine]
    for copy in moved:
        copy.wait()

    all_rows, all_vectors = bands.shape[0], vectors.shape[0]
    tiles, vector_tiles = all_rows // TILE, all_vectors // TILE
    corner = [(i, j) for i in range(tiles) for j in range(i, tiles)]
    corner = {ij: n * TILE for n, ij in enumerate(corner)}
    flat = {(i, j): (i * vector_tiles + j) * TILE for i in range(tiles) for j in range(vector_tiles)}
    for i in range(tiles):
        at = pl.ds(i * TILE, TILE)
        weighted[at, :] = (-(bands[at, :].astype(F32) * gain)).astype(BF16)
    for i in range(tiles):
        at, after = pl.ds(i * TILE, TILE), pl.ds(i * TILE, all_rows - i * TILE)
        sums = dot_rows(bands[at, :], weighted[after, :]) + dot_rows(weighted[at, :], bands[after, :])
        sums = (sums * (-0.5 / total)).astype(BF16)
        for j in range(i, tiles):
            margin_part[pl.ds(corner[i, j], TILE), :] = sums[:, (j - i) * TILE : (j - i + 1) * TILE]
    used = len(corner) * TILE
    if used < margin_part.shape[0]:
        margin_part[used:, :] = jnp.zeros((margin_part.shape[0] - used, LANES), BF16)
    margin_steps = all_reduce(
        count, place, margin_part, margin_half_in, margin_half, margin_first, margin_own, margin_second, margin,
        margin_send, margin_recv,
    )
    next(margin_steps)

    for copy in moved_block:
        copy.wait()
    for i in range(tiles):
        sums = dot_rows(weighted[pl.ds(i * TILE, TILE), :], vectors[...])
        sums = (sums * (1.0 / total)).astype(BF16)
        for j in range(vector_tiles):
            overlap_part[pl.ds(flat[i, j], TILE), :] = sums[:, j * TILE : (j + 1) * TILE]
    used = len(flat) * TILE
    if used < overlap_part.shape[0]:
        overlap_part[used:, :] = jnp.zeros((overlap_part.shape[0] - used, LANES), BF16)
    overlap_steps = all_reduce(
        count, place, overlap_part, overlap_half_in, overlap_half, overlap_first, overlap_own, overlap_second,
        overlap, overlap_send, overlap_recv,
    )
    next(overlap_steps)
    for _ in range(3):
        next(margin_steps)
        next(overlap_steps)
    for i in range(tiles):
        at = pl.ds(i * TILE, TILE)
        work[at, pl.ds(all_rows, cols)] = weighted[at, :].astype(F32)
    next(margin_steps)
    next(margin_steps)

    for (i, j), row in corner.items():
        work[pl.ds(i * TILE, TILE), pl.ds(j * TILE, TILE)] = margin[pl.ds(row, TILE), :].astype(F32)
    edge = all_rows + cols
    segments, applied, early = [], None, None
    for k in range(tiles):
        top = k * TILE
        strips = [work[pl.ds(top + SUB * t, SUB), pl.ds(top, TILE)] for t in range(TILE // SUB)]
        inverse = split(jnp.concatenate(inverse_factor(strips), axis=0))
        first = top + TILE
        if k == 0:
            next(overlap_steps)
        if k == 1:
            next(overlap_steps)
            for (i, j), row in flat.items():
                work[pl.ds(i * TILE, TILE), pl.ds(edge + j * TILE, TILE)] = overlap[pl.ds(row, TILE), :].astype(F32)
            early_inverse, early_lower, early_projector = early
            coupling = dot_split(early_inverse, split(work[pl.ds(0, TILE), pl.ds(edge, all_vectors)]))
            coupling_parts = split(coupling)
            for i in range(1, tiles):
                at = pl.ds(i * TILE, TILE), pl.ds(edge, all_vectors)
                work[at] = work[at] - dot_split(early_lower[i - 1], coupling_parts)
            applied = dot_split(split(coupling.T), early_projector)
        stop = edge if k == 0 else edge + all_vectors
        upper = dot_split(inverse, split(work[pl.ds(top, TILE), pl.ds(first, stop - first)]))
        parts = split(upper)
        lowers = [split(upper[:, i * TILE - first : (i + 1) * TILE - first].T) for i in range(k + 1, tiles)]
        for i in range(k + 1, tiles):
            cut = tuple(part[:, i * TILE - first :] for part in parts)
            at = pl.ds(i * TILE, TILE), pl.ds(i * TILE, stop - i * TILE)
            work[at] = work[at] - dot_split(lowers[i - k - 1], cut)
        base = all_rows - first
        projector = tuple(part[:, base : base + cols] for part in parts)
        ace[pl.ds(top, TILE), :] = projector[0]
        for p in range(count):
            low, high = max(top, p * rows), min(first, (p + 1) * rows)
            if low < high:
                target = pl.ds(low - p * rows, high - low)
                copy = remote(
                    ace.at[pl.ds(low, high - low), :], ace_out.at[target, mine],
                    to_ace.at[len(segments)], from_ace.at[band], p, ga,
                )
                segments.append((p, copy))
                pl.when(band != p)(copy.start)

                @pl.when(band == p)
                def _(low=low, high=high, target=target):
                    ace_out[target, mine] = ace[pl.ds(low, high - low), :]

        if k == 0:
            early = inverse, lowers, projector
        else:
            coupling = split(upper[:, base + cols :].T)
            applied = applied + dot_split(coupling, projector)
    exchange[...] = (-applied).astype(BF16)

    blocks = []
    for d, peer in enumerate(ring(band, count)):
        copy = remote(
            exchange.at[aligned(peer * block_rows, 16, block_rows), :], exchange_out.at[:, mine],
            to_block.at[d], from_block.at[d], peer, ga,
        )
        copy.start()
        blocks.append(copy)
    exchange_out[:, mine] = exchange[vector_rows, :]
    for p, copy in segments:
        pl.when(band != p)(copy.wait_send)
    for q in ring(band, count):
        remote(
            ace.at[pl.ds(0, rows), :], ace_out.at[:, aligned(q * cols, LANES, cols)],
            to_ace.at[0], from_ace.at[q], q, ga,
        ).wait_recv()
    for copy in blocks:
        copy.wait()


def ace_of(count, groups, orbitals, kernel, block_vectors):
    rows, coeffs = orbitals.shape
    block_rows = block_vectors.shape[0]
    bands, vectors, cols = rows * count, block_rows * count, coeffs // count
    tiles = bands // TILE
    dma = pltpu.SemaphoreType.DMA

    def reduced(used):
        pieces = CORES * count
        piece = pl.cdiv(pl.cdiv(used, pieces), 16) * 16
        return [
            pltpu.VMEM((pieces * piece, LANES), BF16),
            pltpu.VMEM((count * piece, LANES), BF16),
            pltpu.VMEM((count - 1, piece, LANES), BF16),
            pltpu.VMEM((count - 1, piece, LANES), BF16),
            pltpu.VMEM((piece, LANES), BF16),
            pltpu.VMEM((count, piece, LANES), BF16),
            pltpu.VMEM((pieces * piece, LANES), BF16),
        ]

    others = dma((count - 1,))
    reducing = dma((4 * count - 2,))
    anywhere = pl.BlockSpec(memory_space=pl.ANY)
    return pl.pallas_call(
        functools.partial(ace_kernel, count, groups),
        out_shape=(
            jax.ShapeDtypeStruct((rows, coeffs), BF16),
            jax.ShapeDtypeStruct((block_rows, coeffs), BF16),
        ),
        in_specs=[anywhere, anywhere, anywhere],
        out_specs=(VMEM, VMEM),
        scratch_shapes=[
            pltpu.VMEM((rows, coeffs), BF16),
            pltpu.VMEM((block_rows, coeffs), BF16),
            pltpu.VMEM((1, coeffs), F32),
            pltpu.VMEM((bands, cols), BF16),
            pltpu.VMEM((vectors, cols), BF16),
            pltpu.VMEM((bands, cols), BF16),
            pltpu.VMEM((bands, bands + cols + vectors), F32),
            pltpu.VMEM((bands, cols), BF16),
            pltpu.VMEM((vectors, cols), BF16),
            *reduced(tiles * (tiles + 1) // 2 * TILE),
            *reduced(tiles * (vectors // TILE) * TILE),
            dma((3,)), others, others, others, others, reducing, reducing, reducing, reducing,
            dma((tiles + count,)), dma((count,)), others, others,
        ],
        compiler_params=pltpu.CompilerParams(
            collective_id=0, has_side_effects=True, vmem_limit_bytes=48 * 2**20
        ),
        name="ace",
    )(orbitals, block_vectors, kernel[None, :])


def solution(mesh):
    placed = (P(("img", "band"), "ga"), P("ga"), P(("img", "band"), "ga"))
    return jax.shard_map(
        functools.partial(ace_of, mesh.shape["band"], mesh.shape["ga"]),
        mesh=mesh,
        in_specs=placed,
        out_specs=(P(("img", "band"), "ga"), P(("img", "band"), "ga")),
        check_vma=False,
    )
```

```python
import functools
import jax
import jax.numpy as jnp
from jax import lax
from jax.experimental import pallas as pl
from jax.experimental.pallas import tpu as pltpu
from jax.sharding import PartitionSpec as P

LANES = 128
SUB = 8
TILE = 128
PANEL = 32
GROUP = 2
CORES = 2
MESH = pl.DeviceIdType.MESH
F32 = jnp.float32
BF16 = jnp.bfloat16
VMEM = pl.BlockSpec(memory_space=pltpu.VMEM)


def row_of(value, index):
    return jnp.broadcast_to(value[index : index + 1, :], value.shape)


def column_of(value, index):
    return jnp.take_along_axis(value, jnp.full(value.shape, index, jnp.int32), axis=1)


def inverse_factor(rows, between=None):
    sub = lax.broadcasted_iota(jnp.int32, (SUB, LANES), 0)
    lane = lax.broadcasted_iota(jnp.int32, (SUB, LANES), 1)
    rows = list(rows)
    count = len(rows)
    per_panel = PANEL // SUB
    size = GROUP * SUB
    done = []
    for begin in range(0, count, GROUP):
        first = begin * SUB
        last = (begin // per_panel + 1) * per_panel
        inside = (lane >= first) & (lane < first + size)
        strips = rows[begin : begin + GROUP]
        columns = [[column_of(strip, first + k) for k in range(size)] for strip in strips]
        solved = [
            jnp.where(inside, jnp.where(lane - first == sub + s * SUB, 1.0, 0.0), strips[s])
            for s in range(GROUP)
        ]
        forward = list(solved)
        scale = [jnp.ones((SUB, LANES), F32)] * GROUP
        diagonal = [jnp.ones((SUB, LANES), F32)] * GROUP
        for j in range(size):
            js, jj = divmod(j, SUB)
            value = row_of(columns[js][j], jj)
            pivot = 1.0 / value
            here = sub == jj
            scale[js] = jnp.where(here, pivot, scale[js])
            diagonal[js] = jnp.where(here, value, diagonal[js])
            factor = [columns[s][j] * pivot for s in range(GROUP)]
            factor[js] = jnp.where(here, 0.0, factor[js])
            for k in range(j + 1, size):
                row = row_of(columns[js][k], jj)
                for s in range(GROUP):
                    columns[s][k] = columns[s][k] - factor[s] * row
            row = row_of(forward[js], jj)
            if jj < SUB - 1:
                forward[js] = forward[js] - jnp.where(sub > jj, factor[js], 0.0) * row
            for s in range(js + 1, GROUP):
                forward[s] = forward[s] - factor[s] * row
            row = row_of(solved[js], jj)
            for s in range(GROUP):
                solved[s] = solved[s] - factor[s] * row
        for s in range(GROUP):
            kept = forward[s] * lax.rsqrt(diagonal[s])
            stop = first + (s + 1) * SUB
            if stop < last * SUB:
                kept = jnp.where((lane < stop) | (lane >= last * SUB), kept, 0.0)
            done.append(kept)
        after = begin + GROUP
        if after < last:
            solved_rows = [row_of(solved[s] * scale[s], jj) for s in range(GROUP) for jj in range(SUB)]
            for r in range(after, last):
                old = rows[r]
                total = jnp.where(inside, 0.0, old)
                terms = [column_of(old, first + j) * solved_rows[j] for j in range(size)]
                while len(terms) > 1:
                    terms = [terms[i] + terms[i + 1] for i in range(0, len(terms), 2)]
                rows[r] = total - terms[0]
        elif last < count:
            if between is not None and last == count - per_panel:
                between()
            start = last - per_panel
            upper = jnp.concatenate(done[start:last], axis=0)
            product = dot_split(split(upper.T), split(upper))
            gone = (lane >= start * SUB) & (lane < last * SUB)
            for r in range(last, count):
                rows[r] = jnp.where(gone, 0.0, rows[r]) - product[r * SUB : r * SUB + SUB, :]
    return [jnp.where(lane < (t + 1) * SUB, done[t], 0.0) for t in range(count)]


def split(value):
    high = value.astype(BF16)
    return high, (value - high.astype(F32)).astype(BF16)


def dot(left, right):
    return lax.dot_general(left, right, (((1,), (0,)), ((), ())), preferred_element_type=F32)


def dot_rows(left, right):
    return lax.dot_general(left, right, (((1,), (1,)), ((), ())), preferred_element_type=F32)


def dot_split(left, right):
    (lh, ll), (rh, rl) = left, right
    return dot(lh, rh) + dot(lh, rl) + dot(ll, rh)


def remote(src, dst, send, recv, band, ga):
    return pltpu.make_async_remote_copy(
        src_ref=src,
        dst_ref=dst,
        send_sem=send,
        recv_sem=recv,
        device_id={"band": band, "ga": ga},
        device_id_type=MESH,
    )


def meet(devices):
    barrier = pltpu.get_barrier_semaphore()
    for band, ga in devices:
        pl.semaphore_signal(barrier, inc=1, device_id={"band": band, "ga": ga}, device_id_type=MESH)
    pl.semaphore_wait(barrier, len(devices))


def aligned(start, step, size):
    return pl.ds(pl.multiple_of(start, step), size)


def ring(position, count):
    return [(position + d) % count for d in range(1, count)]


def all_reduce(count, place, part, half_in, half, first_in, own, second_in, out, send, recv):
    core, here, there, along_first, along_second, pair = place
    piece = part.shape[0] // (CORES * count)
    size = piece * count
    pair_at, first_at, second_at, spread_at, give_at = 0, 1, count, 2 * count - 1, 3 * count - 2
    steps = range(1, count)

    def piece_at(q):
        return aligned((core * count + q) * piece, 16, piece)

    def copy_to(src, dst, sem, device):
        copy = remote(src, dst, send.at[sem], recv.at[sem], *device)
        copy.start()
        return copy

    swap = copy_to(part.at[aligned((1 - core) * size, 16, size), :], half_in, pair_at, pair)
    yield
    swap.wait()
    copies = []
    for d in range(1, count + 1):
        q = (here + d) % count
        theirs = half_in[aligned(q * piece, 16, piece), :].astype(F32)
        summed = part[piece_at(q), :].astype(F32) + theirs
        if d < count:
            half[d - 1] = summed.astype(BF16)
            copies.append(copy_to(half.at[d - 1], first_in.at[d - 1], first_at + d - 1, along_first(q)))
    yield
    for d, copy in enumerate(copies):
        copy.wait()
        summed = summed + first_in[d].astype(F32)
    own[...] = summed.astype(BF16)
    copies = []
    for d in steps:
        device = along_second((there + d) % count)
        copies.append(copy_to(own, second_in.at[there], second_at + d - 1, device))
    second_in[there] = own[...]
    yield
    for copy in copies:
        copy.wait()
    summed = second_in[0].astype(F32)
    for q in steps:
        summed = summed + second_in[q].astype(F32)
    out[piece_at(here), :] = summed.astype(BF16)
    copies, given = [], []

    def pass_on(slot, q):
        at = out.at[piece_at(q), :]
        given.append(copy_to(at, at, give_at + slot, pair))

    for d in steps:
        at = out.at[piece_at(here), :]
        copies.append(copy_to(at, at, spread_at + d - 1, along_first((here + d) % count)))
    pass_on(0, here)
    yield
    for d in steps:
        copies[d - 1].wait_recv()
        pass_on(d, (here - d + count) % count)
    yield
    for copy in copies:
        copy.wait_send()
    for copy in given:
        copy.wait()
    yield


def ace_kernel(
    count, groups, orbitals_ref, block_ref, kernel_ref, ace_out, exchange_out,
    orbitals, block, gains, bands, vectors, weighted, work, ace, exchange,
    *rest,
):
    head_refs, tail_refs, overlap_refs = rest[:7], rest[7:14], rest[14:21]
    (load, to_bands, from_bands, to_vectors, from_vectors, head_send, head_recv, tail_send, tail_recv,
     overlap_send, overlap_recv, to_ace, from_ace, to_block, from_block) = rest[21:]
    band, ga = lax.axis_index("band"), lax.axis_index("ga")
    line, core = ga // CORES, ga % CORES
    rows, cols = orbitals.shape[0], weighted.shape[1]
    block_rows = block.shape[0]
    total = orbitals.shape[1] * groups
    here = (1 - core) * band + core * line
    there = (1 - core) * line + core * band

    def along_first(q):
        return (1 - core) * q + core * band, CORES * ((1 - core) * line + core * q) + core

    def along_second(q):
        return (1 - core) * band + core * q, CORES * ((1 - core) * q + core * line) + core

    pair = (band, CORES * line + 1 - core)
    place = (core, here, there, along_first, along_second, pair)

    loads = [
        pltpu.make_async_copy(orbitals_ref, orbitals, load.at[0]),
        pltpu.make_async_copy(block_ref, block, load.at[1]),
        pltpu.make_async_copy(kernel_ref, gains, load.at[2]),
    ]
    for copy in loads:
        copy.start()
    meet(
        [along_first(q) for q in ring(here, count)]
        + [along_second(q) for q in ring(there, count)]
        + [pair]
    )
    for copy in loads:
        copy.wait()

    mine = aligned(band * cols, LANES, cols)
    band_rows = aligned(band * rows, 16, rows)
    vector_rows = aligned(band * block_rows, 16, block_rows)
    moved, moved_block = [], []
    for d, peer in enumerate(ring(band, count)):
        theirs = aligned(peer * cols, LANES, cols)
        moved.append(
            remote(orbitals.at[:, theirs], bands.at[band_rows, :], to_bands.at[d], from_bands.at[d], peer, ga)
        )
        moved_block.append(
            remote(block.at[:, theirs], vectors.at[vector_rows, :], to_vectors.at[d], from_vectors.at[d], peer, ga)
        )
    for copy in moved + moved_block:
        copy.start()
    bands[band_rows, :] = orbitals[:, mine]
    vectors[vector_rows, :] = block[:, mine]
    gain = gains[:, mine]
    for copy in moved:
        copy.wait()

    all_rows, all_vectors = bands.shape[0], vectors.shape[0]
    tiles, vector_tiles = all_rows // TILE, all_vectors // TILE
    head = {(0, j): j * TILE for j in range(tiles)}
    tail = [(i, j) for i in range(1, tiles) for j in range(i, tiles)]
    tail = {ij: n * TILE for n, ij in enumerate(tail)}
    flat = {(i, j): (i * vector_tiles + j) * TILE for i in range(tiles) for j in range(vector_tiles)}

    def clear_after(where, part):
        used = len(where) * TILE
        if used < part.shape[0]:
            part[used:, :] = jnp.zeros((part.shape[0] - used, LANES), BF16)

    def margin_rows(i, where, part):
        at, after = pl.ds(i * TILE, TILE), pl.ds(i * TILE, all_rows - i * TILE)
        sums = dot_rows(bands[at, :], weighted[after, :]) + dot_rows(weighted[at, :], bands[after, :])
        sums = (sums * (-0.5 / total)).astype(BF16)
        for j in range(i, tiles):
            part[pl.ds(where[i, j], TILE), :] = sums[:, (j - i) * TILE : (j - i + 1) * TILE]

    for i in range(tiles):
        at = pl.ds(i * TILE, TILE)
        weighted[at, :] = (-(bands[at, :].astype(F32) * gain)).astype(BF16)
    margin_rows(0, head, head_refs[0])
    clear_after(head, head_refs[0])
    head_steps = all_reduce(count, place, *head_refs, head_send, head_recv)
    next(head_steps)
    for i in range(1, tiles):
        margin_rows(i, tail, tail_refs[0])
    clear_after(tail, tail_refs[0])
    tail_steps = all_reduce(count, place, *tail_refs, tail_send, tail_recv)
    next(tail_steps)
    next(head_steps)
    for copy in moved_block:
        copy.wait()
    for i in range(tiles):
        sums = dot_rows(weighted[pl.ds(i * TILE, TILE), :], vectors[...])
        sums = (sums * (1.0 / total)).astype(BF16)
        for j in range(vector_tiles):
            overlap_refs[0][pl.ds(flat[i, j], TILE), :] = sums[:, j * TILE : (j + 1) * TILE]
    clear_after(flat, overlap_refs[0])
    overlap_steps = all_reduce(count, place, *overlap_refs, overlap_send, overlap_recv)
    next(overlap_steps)
    next(tail_steps)
    next(head_steps)
    next(overlap_steps)
    next(tail_steps)
    next(head_steps)
    next(overlap_steps)
    next(tail_steps)
    for i in range(tiles):
        at = pl.ds(i * TILE, TILE)
        work[at, pl.ds(all_rows, cols)] = weighted[at, :].astype(F32)
    next(head_steps)
    next(overlap_steps)
    next(head_steps)

    def unpack(where, out, column):
        for (i, j), row in where.items():
            work[pl.ds(i * TILE, TILE), pl.ds(column + j * TILE, TILE)] = out[pl.ds(row, TILE), :].astype(F32)

    def factored(value, between=None):
        strips = [value[SUB * t : SUB * (t + 1), :] for t in range(TILE // SUB)]
        return split(jnp.concatenate(inverse_factor(strips, between), axis=0))

    unpack(head, head_refs[-1], 0)
    inverse = factored(work[pl.ds(0, TILE), pl.ds(0, TILE)], lambda: next(tail_steps))
    next(tail_steps)
    next(overlap_steps)
    unpack(tail, tail_refs[-1], 0)
    edge = all_rows + cols
    segments, applied, early = [], None, None
    for k in range(tiles):
        top = k * TILE
        first = top + TILE
        ours = pl.ds(top, TILE)
        if k == 1:
            next(overlap_steps)
        ending = k == tiles - 1
        if not ending:
            at = pl.ds(first, TILE)
            ahead = split(dot_split(inverse, split(work[ours, at])))
            lower = split((ahead[0].astype(F32) + ahead[1].astype(F32)).T)
            following = factored(work[at, at] - dot_split(lower, ahead))
            lowers = [lower]
        else:
            lowers = []
        if k == 1:
            unpack(flat, overlap_refs[-1], edge)
            early_inverse, early_lowers, early_projector = early
            coupling = dot_split(early_inverse, split(work[pl.ds(0, TILE), pl.ds(edge, all_vectors)]))
            coupling_parts = split(coupling)
            for i in range(1, tiles):
                at = pl.ds(i * TILE, TILE), pl.ds(edge, all_vectors)
                work[at] = work[at] - dot_split(early_lowers[i - 1], coupling_parts)
            applied = dot_split(split(coupling.T), early_projector)
        start = min(first + TILE, all_rows)
        stop = edge if k == 0 else edge + all_vectors
        upper = dot_split(inverse, split(work[ours, pl.ds(start, stop - start)]))
        parts = split(upper)
        for i in range(k + 2, tiles):
            lowers.append(split(upper[:, i * TILE - start : (i + 1) * TILE - start].T))
        for i in range(k + 1, tiles):
            low = max(i * TILE, start)
            cut = tuple(part[:, low - start :] for part in parts)
            at = pl.ds(i * TILE, TILE), pl.ds(low, stop - low)
            work[at] = work[at] - dot_split(lowers[i - k - 1], cut)
        base = all_rows - start
        projector = tuple(part[:, base : base + cols] for part in parts)
        ace[ours, :] = projector[0]
        for p in range(count):
            low, high = max(top, p * rows), min(first, (p + 1) * rows)
            if low < high:
                target = pl.ds(low - p * rows, high - low)
                copy = remote(
                    ace.at[pl.ds(low, high - low), :], ace_out.at[target, mine],
                    to_ace.at[len(segments)], from_ace.at[band], p, ga,
                )
                segments.append((p, copy))
                pl.when(band != p)(copy.start)

                @pl.when(band == p)
                def _(low=low, high=high, target=target):
                    ace_out[target, mine] = ace[pl.ds(low, high - low), :]

        if k == 0:
            early = inverse, lowers, projector
        else:
            coupling = split(upper[:, base + cols :].T)
            applied = applied + dot_split(coupling, projector)
        if not ending:
            inverse = following
    exchange[...] = (-applied).astype(BF16)

    blocks = []
    for d, peer in enumerate(ring(band, count)):
        copy = remote(
            exchange.at[aligned(peer * block_rows, 16, block_rows), :], exchange_out.at[:, mine],
            to_block.at[d], from_block.at[d], peer, ga,
        )
        copy.start()
        blocks.append(copy)
    exchange_out[:, mine] = exchange[vector_rows, :]
    for p, copy in segments:
        pl.when(band != p)(copy.wait_send)
    for q in ring(band, count):
        remote(
            ace.at[pl.ds(0, rows), :], ace_out.at[:, aligned(q * cols, LANES, cols)],
            to_ace.at[0], from_ace.at[q], q, ga,
        ).wait_recv()
    for copy in blocks:
        copy.wait()


def ace_of(count, groups, orbitals, kernel, block_vectors):
    rows, coeffs = orbitals.shape
    block_rows = block_vectors.shape[0]
    bands, vectors, cols = rows * count, block_rows * count, coeffs // count
    tiles = bands // TILE
    dma = pltpu.SemaphoreType.DMA

    def reduced(used):
        pieces = CORES * count
        piece = pl.cdiv(pl.cdiv(used, pieces), 16) * 16
        return [
            pltpu.VMEM((pieces * piece, LANES), BF16),
            pltpu.VMEM((count * piece, LANES), BF16),
            pltpu.VMEM((count - 1, piece, LANES), BF16),
            pltpu.VMEM((count - 1, piece, LANES), BF16),
            pltpu.VMEM((piece, LANES), BF16),
            pltpu.VMEM((count, piece, LANES), BF16),
            pltpu.VMEM((pieces * piece, LANES), BF16),
        ]

    others = dma((count - 1,))
    reducing = dma((4 * count - 2,))
    anywhere = pl.BlockSpec(memory_space=pl.ANY)
    return pl.pallas_call(
        functools.partial(ace_kernel, count, groups),
        out_shape=(
            jax.ShapeDtypeStruct((rows, coeffs), BF16),
            jax.ShapeDtypeStruct((block_rows, coeffs), BF16),
        ),
        in_specs=[anywhere, anywhere, anywhere],
        out_specs=(VMEM, VMEM),
        scratch_shapes=[
            pltpu.VMEM((rows, coeffs), BF16),
            pltpu.VMEM((block_rows, coeffs), BF16),
            pltpu.VMEM((1, coeffs), F32),
            pltpu.VMEM((bands, cols), BF16),
            pltpu.VMEM((vectors, cols), BF16),
            pltpu.VMEM((bands, cols), BF16),
            pltpu.VMEM((bands, bands + cols + vectors), F32),
            pltpu.VMEM((bands, cols), BF16),
            pltpu.VMEM((vectors, cols), BF16),
            *reduced(tiles * TILE),
            *reduced(tiles * (tiles - 1) // 2 * TILE),
            *reduced(tiles * (vectors // TILE) * TILE),
            dma((3,)), others, others, others, others,
            reducing, reducing, reducing, reducing, reducing, reducing,
            dma((tiles + count,)), dma((count,)), others, others,
        ],
        compiler_params=pltpu.CompilerParams(
            collective_id=0, has_side_effects=True, vmem_limit_bytes=62 * 2**20
        ),
        name="ace",
    )(orbitals, block_vectors, kernel[None, :])


def solution(mesh):
    placed = (P(("img", "band"), "ga"), P("ga"), P(("img", "band"), "ga"))
    return jax.shard_map(
        functools.partial(ace_of, mesh.shape["band"], mesh.shape["ga"]),
        mesh=mesh,
        in_specs=placed,
        out_specs=(P(("img", "band"), "ga"), P(("img", "band"), "ga")),
        check_vma=False,
    )
```

```python
import functools
import jax
import jax.numpy as jnp
from jax import lax
from jax.experimental import pallas as pl
from jax.experimental.pallas import tpu as pltpu
from jax.sharding import PartitionSpec as P

LANES = 128
SUB = 8
TILE = 128
PANEL = 32
GROUP = 2
CORES = 2
MESH = pl.DeviceIdType.MESH
F32 = jnp.float32
BF16 = jnp.bfloat16
VMEM = pl.BlockSpec(memory_space=pltpu.VMEM)


def row_of(value, index):
    return jnp.broadcast_to(value[index : index + 1, :], value.shape)


def column_of(value, index):
    return jnp.take_along_axis(value, jnp.full(value.shape, index, jnp.int32), axis=1)


def inverse_factor(rows, between=None):
    sub = lax.broadcasted_iota(jnp.int32, (SUB, LANES), 0)
    lane = lax.broadcasted_iota(jnp.int32, (SUB, LANES), 1)
    rows = list(rows)
    count = len(rows)
    per_panel = PANEL // SUB
    size = GROUP * SUB
    done = []
    for begin in range(0, count, GROUP):
        first = begin * SUB
        last = (begin // per_panel + 1) * per_panel
        inside = (lane >= first) & (lane < first + size)
        strips = rows[begin : begin + GROUP]
        columns = [[column_of(strip, first + k) for k in range(size)] for strip in strips]
        solved = [
            jnp.where(inside, jnp.where(lane - first == sub + s * SUB, 1.0, 0.0), strips[s])
            for s in range(GROUP)
        ]
        forward = list(solved)
        scale = [jnp.ones((SUB, LANES), F32)] * GROUP
        diagonal = [jnp.ones((SUB, LANES), F32)] * GROUP
        for j in range(size):
            js, jj = divmod(j, SUB)
            value = row_of(columns[js][j], jj)
            pivot = 1.0 / value
            here = sub == jj
            scale[js] = jnp.where(here, pivot, scale[js])
            diagonal[js] = jnp.where(here, value, diagonal[js])
            factor = [columns[s][j] * pivot for s in range(GROUP)]
            factor[js] = jnp.where(here, 0.0, factor[js])
            for k in range(j + 1, size):
                row = row_of(columns[js][k], jj)
                for s in range(GROUP):
                    columns[s][k] = columns[s][k] - factor[s] * row
            row = row_of(forward[js], jj)
            if jj < SUB - 1:
                forward[js] = forward[js] - jnp.where(sub > jj, factor[js], 0.0) * row
            for s in range(js + 1, GROUP):
                forward[s] = forward[s] - factor[s] * row
            row = row_of(solved[js], jj)
            for s in range(GROUP):
                solved[s] = solved[s] - factor[s] * row
        for s in range(GROUP):
            kept = forward[s] * lax.rsqrt(diagonal[s])
            stop = first + (s + 1) * SUB
            if stop < last * SUB:
                kept = jnp.where((lane < stop) | (lane >= last * SUB), kept, 0.0)
            done.append(kept)
        after = begin + GROUP
        if after < last:
            solved_rows = [row_of(solved[s] * scale[s], jj) for s in range(GROUP) for jj in range(SUB)]
            for r in range(after, last):
                old = rows[r]
                total = jnp.where(inside, 0.0, old)
                terms = [column_of(old, first + j) * solved_rows[j] for j in range(size)]
                while len(terms) > 1:
                    terms = [terms[i] + terms[i + 1] for i in range(0, len(terms), 2)]
                rows[r] = total - terms[0]
        elif last < count:
            if between is not None and last == count - per_panel:
                between()
            start = last - per_panel
            upper = jnp.concatenate(done[start:last], axis=0)
            high, low = split(upper)
            product = lax.dot_general(
                jnp.concatenate([high, high, low], axis=0),
                jnp.concatenate([high, low, high], axis=0),
                (((0,), (0,)), ((), ())),
                preferred_element_type=F32,
            )
            gone = (lane >= start * SUB) & (lane < last * SUB)
            for r in range(last, count):
                rows[r] = jnp.where(gone, 0.0, rows[r]) - product[r * SUB : r * SUB + SUB, :]
    return [jnp.where(lane < (t + 1) * SUB, done[t], 0.0) for t in range(count)]


def split(value):
    high = value.astype(BF16)
    return high, (value - high.astype(F32)).astype(BF16)


def dot(left, right):
    return lax.dot_general(left, right, (((1,), (0,)), ((), ())), preferred_element_type=F32)


def dot_rows(left, right):
    return lax.dot_general(left, right, (((1,), (1,)), ((), ())), preferred_element_type=F32)


def dot_split(left, right):
    (lh, ll), (rh, rl) = left, right
    return dot(jnp.concatenate([lh, lh, ll], axis=1), jnp.concatenate([rh, rl, rh], axis=0))


def remote(src, dst, send, recv, band, ga):
    return pltpu.make_async_remote_copy(
        src_ref=src,
        dst_ref=dst,
        send_sem=send,
        recv_sem=recv,
        device_id={"band": band, "ga": ga},
        device_id_type=MESH,
    )


def meet(devices):
    barrier = pltpu.get_barrier_semaphore()
    for band, ga in devices:
        pl.semaphore_signal(barrier, inc=1, device_id={"band": band, "ga": ga}, device_id_type=MESH)
    pl.semaphore_wait(barrier, len(devices))


def aligned(start, step, size):
    return pl.ds(pl.multiple_of(start, step), size)


def ring(position, count):
    return [(position + d) % count for d in range(1, count)]


def all_reduce(count, place, part, half_in, half, first_in, own, second_in, out, send, recv):
    core, here, there, along_first, along_second, pair = place
    piece = part.shape[0] // (CORES * count)
    size = piece * count
    pair_at, first_at, second_at, spread_at, give_at = 0, 1, count, 2 * count - 1, 3 * count - 2
    steps = range(1, count)

    def piece_at(q):
        return aligned((core * count + q) * piece, 16, piece)

    def copy_to(src, dst, sem, device):
        copy = remote(src, dst, send.at[sem], recv.at[sem], *device)
        copy.start()
        return copy

    swap = copy_to(part.at[aligned((1 - core) * size, 16, size), :], half_in, pair_at, pair)
    yield
    swap.wait()
    copies = []
    for d in range(1, count + 1):
        q = (here + d) % count
        theirs = half_in[aligned(q * piece, 16, piece), :].astype(F32)
        summed = part[piece_at(q), :].astype(F32) + theirs
        if d < count:
            half[d - 1] = summed.astype(BF16)
            copies.append(copy_to(half.at[d - 1], first_in.at[d - 1], first_at + d - 1, along_first(q)))
    yield
    for d, copy in enumerate(copies):
        copy.wait()
        summed = summed + first_in[d].astype(F32)
    own[...] = summed.astype(BF16)
    copies = []
    for d in steps:
        device = along_second((there + d) % count)
        copies.append(copy_to(own, second_in.at[there], second_at + d - 1, device))
    second_in[there] = own[...]
    yield
    for copy in copies:
        copy.wait()
    summed = second_in[0].astype(F32)
    for q in steps:
        summed = summed + second_in[q].astype(F32)
    out[piece_at(here), :] = summed.astype(BF16)
    copies, given = [], []

    def pass_on(slot, q):
        at = out.at[piece_at(q), :]
        given.append(copy_to(at, at, give_at + slot, pair))

    for d in steps:
        at = out.at[piece_at(here), :]
        copies.append(copy_to(at, at, spread_at + d - 1, along_first((here + d) % count)))
    pass_on(0, here)
    yield
    for d in steps:
        copies[d - 1].wait_recv()
        pass_on(d, (here - d + count) % count)
    yield
    for copy in copies:
        copy.wait_send()
    for copy in given:
        copy.wait()
    yield


def ace_kernel(
    count, groups, orbitals_ref, block_ref, kernel_ref, ace_out, exchange_out,
    orbitals, block, gains, bands, vectors, weighted, work, ace, exchange,
    *rest,
):
    head_refs, tail_refs, overlap_refs = rest[:7], rest[7:14], rest[14:21]
    (load, to_bands, from_bands, to_vectors, from_vectors, head_send, head_recv, tail_send, tail_recv,
     overlap_send, overlap_recv, to_ace, from_ace, to_block, from_block) = rest[21:]
    band, ga = lax.axis_index("band"), lax.axis_index("ga")
    line, core = ga // CORES, ga % CORES
    rows, cols = orbitals.shape[0], weighted.shape[1]
    block_rows = block.shape[0]
    total = orbitals.shape[1] * groups
    here = (1 - core) * band + core * line
    there = (1 - core) * line + core * band

    def along_first(q):
        return (1 - core) * q + core * band, CORES * ((1 - core) * line + core * q) + core

    def along_second(q):
        return (1 - core) * band + core * q, CORES * ((1 - core) * q + core * line) + core

    pair = (band, CORES * line + 1 - core)
    place = (core, here, there, along_first, along_second, pair)

    loads = [
        pltpu.make_async_copy(orbitals_ref, orbitals, load.at[0]),
        pltpu.make_async_copy(block_ref, block, load.at[1]),
        pltpu.make_async_copy(kernel_ref, gains, load.at[2]),
    ]
    for copy in loads:
        copy.start()
    meet(
        [along_first(q) for q in ring(here, count)]
        + [along_second(q) for q in ring(there, count)]
        + [pair]
    )
    for copy in loads:
        copy.wait()

    mine = aligned(band * cols, LANES, cols)
    band_rows = aligned(band * rows, 16, rows)
    vector_rows = aligned(band * block_rows, 16, block_rows)
    moved, moved_block = [], []
    for d, peer in enumerate(ring(band, count)):
        theirs = aligned(peer * cols, LANES, cols)
        moved.append(
            remote(orbitals.at[:, theirs], bands.at[band_rows, :], to_bands.at[d], from_bands.at[d], peer, ga)
        )
        moved_block.append(
            remote(block.at[:, theirs], vectors.at[vector_rows, :], to_vectors.at[d], from_vectors.at[d], peer, ga)
        )
    for copy in moved + moved_block:
        copy.start()
    bands[band_rows, :] = orbitals[:, mine]
    vectors[vector_rows, :] = block[:, mine]
    gain = gains[:, mine]
    for copy in moved:
        copy.wait()

    all_rows, all_vectors = bands.shape[0], vectors.shape[0]
    tiles, vector_tiles = all_rows // TILE, all_vectors // TILE
    head = {(0, j): j * TILE for j in range(tiles)}
    tail = [(i, j) for i in range(1, tiles) for j in range(i, tiles)]
    tail = {ij: n * TILE for n, ij in enumerate(tail)}
    flat = {(i, j): (i * vector_tiles + j) * TILE for i in range(tiles) for j in range(vector_tiles)}

    def clear_after(where, part):
        used = len(where) * TILE
        if used < part.shape[0]:
            part[used:, :] = jnp.zeros((part.shape[0] - used, LANES), BF16)

    def margin_rows(i, where, part):
        at, after = pl.ds(i * TILE, TILE), pl.ds(i * TILE, all_rows - i * TILE)
        sums = dot_rows(bands[at, :], weighted[after, :]) + dot_rows(weighted[at, :], bands[after, :])
        sums = (sums * (-0.5 / total)).astype(BF16)
        for j in range(i, tiles):
            part[pl.ds(where[i, j], TILE), :] = sums[:, (j - i) * TILE : (j - i + 1) * TILE]

    for i in range(tiles):
        at = pl.ds(i * TILE, TILE)
        weighted[at, :] = (-(bands[at, :].astype(F32) * gain)).astype(BF16)
    margin_rows(0, head, head_refs[0])
    clear_after(head, head_refs[0])
    head_steps = all_reduce(count, place, *head_refs, head_send, head_recv)
    next(head_steps)
    for i in range(1, tiles):
        margin_rows(i, tail, tail_refs[0])
    clear_after(tail, tail_refs[0])
    tail_steps = all_reduce(count, place, *tail_refs, tail_send, tail_recv)
    next(tail_steps)
    next(head_steps)
    for copy in moved_block:
        copy.wait()
    for i in range(tiles):
        sums = dot_rows(weighted[pl.ds(i * TILE, TILE), :], vectors[...])
        sums = (sums * (1.0 / total)).astype(BF16)
        for j in range(vector_tiles):
            overlap_refs[0][pl.ds(flat[i, j], TILE), :] = sums[:, j * TILE : (j + 1) * TILE]
    clear_after(flat, overlap_refs[0])
    overlap_steps = all_reduce(count, place, *overlap_refs, overlap_send, overlap_recv)
    next(overlap_steps)
    next(tail_steps)
    next(head_steps)
    next(overlap_steps)
    next(tail_steps)
    next(head_steps)
    next(overlap_steps)
    next(tail_steps)
    for i in range(tiles):
        at = pl.ds(i * TILE, TILE)
        work[at, pl.ds(all_rows, cols)] = weighted[at, :].astype(F32)
    next(head_steps)
    next(overlap_steps)
    next(head_steps)

    def unpack(where, out, column):
        for (i, j), row in where.items():
            work[pl.ds(i * TILE, TILE), pl.ds(column + j * TILE, TILE)] = out[pl.ds(row, TILE), :].astype(F32)

    def factored(value, between=None):
        strips = [value[SUB * t : SUB * (t + 1), :] for t in range(TILE // SUB)]
        return split(jnp.concatenate(inverse_factor(strips, between), axis=0))

    unpack(head, head_refs[-1], 0)
    inverse = factored(work[pl.ds(0, TILE), pl.ds(0, TILE)], lambda: next(tail_steps))
    next(tail_steps)
    next(overlap_steps)
    unpack(tail, tail_refs[-1], 0)
    edge = all_rows + cols
    segments, applied, early = [], None, None
    for k in range(tiles):
        top = k * TILE
        first = top + TILE
        ours = pl.ds(top, TILE)
        if k == 1:
            next(overlap_steps)
        ending = k == tiles - 1
        if not ending:
            at = pl.ds(first, TILE)
            ahead = split(dot_split(inverse, split(work[ours, at])))
            lower = split((ahead[0].astype(F32) + ahead[1].astype(F32)).T)
            value = work[at, at] - dot_split(lower, ahead)
            following = factored(value) if k < tiles - 2 else None
            lowers = [lower]
        else:
            lowers = []
        if k == 1:
            unpack(flat, overlap_refs[-1], edge)
            early_inverse, early_lowers, early_projector = early
            coupling = dot_split(early_inverse, split(work[pl.ds(0, TILE), pl.ds(edge, all_vectors)]))
            coupling_parts = split(coupling)
            for i in range(1, tiles):
                at = pl.ds(i * TILE, TILE), pl.ds(edge, all_vectors)
                work[at] = work[at] - dot_split(early_lowers[i - 1], coupling_parts)
            applied = dot_split(split(coupling.T), early_projector)
        start = min(first + TILE, all_rows)
        stop = edge if k == 0 else edge + all_vectors
        upper = dot_split(inverse, split(work[ours, pl.ds(start, stop - start)]))
        parts = split(upper)
        for i in range(k + 2, tiles):
            lowers.append(split(upper[:, i * TILE - start : (i + 1) * TILE - start].T))
        for i in range(k + 1, tiles):
            low = max(i * TILE, start)
            cut = tuple(part[:, low - start :] for part in parts)
            at = pl.ds(i * TILE, TILE), pl.ds(low, stop - low)
            work[at] = work[at] - dot_split(lowers[i - k - 1], cut)
        base = all_rows - start
        projector = tuple(part[:, base : base + cols] for part in parts)
        ace[ours, :] = projector[0]
        for p in range(count):
            low, high = max(top, p * rows), min(first, (p + 1) * rows)
            if low < high:
                target = pl.ds(low - p * rows, high - low)
                copy = remote(
                    ace.at[pl.ds(low, high - low), :], ace_out.at[target, mine],
                    to_ace.at[len(segments)], from_ace.at[band], p, ga,
                )
                segments.append((p, copy))
                pl.when(band != p)(copy.start)

                @pl.when(band == p)
                def _(low=low, high=high, target=target):
                    ace_out[target, mine] = ace[pl.ds(low, high - low), :]

        if k == 0:
            early = inverse, lowers, projector
        else:
            coupling = split(upper[:, base + cols :].T)
            applied = applied + dot_split(coupling, projector)
        if not ending:
            inverse = factored(value) if following is None else following
    exchange[...] = (-applied).astype(BF16)

    blocks = []
    for d, peer in enumerate(ring(band, count)):
        copy = remote(
            exchange.at[aligned(peer * block_rows, 16, block_rows), :], exchange_out.at[:, mine],
            to_block.at[d], from_block.at[d], peer, ga,
        )
        copy.start()
        blocks.append(copy)
    exchange_out[:, mine] = exchange[vector_rows, :]
    for p, copy in segments:
        pl.when(band != p)(copy.wait_send)
    for q in ring(band, count):
        remote(
            ace.at[pl.ds(0, rows), :], ace_out.at[:, aligned(q * cols, LANES, cols)],
            to_ace.at[0], from_ace.at[q], q, ga,
        ).wait_recv()
    for copy in blocks:
        copy.wait()


def ace_of(count, groups, orbitals, kernel, block_vectors):
    rows, coeffs = orbitals.shape
    block_rows = block_vectors.shape[0]
    bands, vectors, cols = rows * count, block_rows * count, coeffs // count
    tiles = bands // TILE
    dma = pltpu.SemaphoreType.DMA

    def reduced(used):
        pieces = CORES * count
        piece = pl.cdiv(pl.cdiv(used, pieces), 16) * 16
        return [
            pltpu.VMEM((pieces * piece, LANES), BF16),
            pltpu.VMEM((count * piece, LANES), BF16),
            pltpu.VMEM((count - 1, piece, LANES), BF16),
            pltpu.VMEM((count - 1, piece, LANES), BF16),
            pltpu.VMEM((piece, LANES), BF16),
            pltpu.VMEM((count, piece, LANES), BF16),
            pltpu.VMEM((pieces * piece, LANES), BF16),
        ]

    others = dma((count - 1,))
    reducing = dma((4 * count - 2,))
    anywhere = pl.BlockSpec(memory_space=pl.ANY)
    return pl.pallas_call(
        functools.partial(ace_kernel, count, groups),
        out_shape=(
            jax.ShapeDtypeStruct((rows, coeffs), BF16),
            jax.ShapeDtypeStruct((block_rows, coeffs), BF16),
        ),
        in_specs=[anywhere, anywhere, anywhere],
        out_specs=(VMEM, VMEM),
        scratch_shapes=[
            pltpu.VMEM((rows, coeffs), BF16),
            pltpu.VMEM((block_rows, coeffs), BF16),
            pltpu.VMEM((1, coeffs), F32),
            pltpu.VMEM((bands, cols), BF16),
            pltpu.VMEM((vectors, cols), BF16),
            pltpu.VMEM((bands, cols), BF16),
            pltpu.VMEM((bands, bands + cols + vectors), F32),
            pltpu.VMEM((bands, cols), BF16),
            pltpu.VMEM((vectors, cols), BF16),
            *reduced(tiles * TILE),
            *reduced(tiles * (tiles - 1) // 2 * TILE),
            *reduced(tiles * (vectors // TILE) * TILE),
            dma((3,)), others, others, others, others,
            reducing, reducing, reducing, reducing, reducing, reducing,
            dma((tiles + count,)), dma((count,)), others, others,
        ],
        compiler_params=pltpu.CompilerParams(
            collective_id=0, has_side_effects=True, vmem_limit_bytes=62 * 2**20
        ),
        name="ace",
    )(orbitals, block_vectors, kernel[None, :])


def solution(mesh):
    placed = (P(("img", "band"), "ga"), P("ga"), P(("img", "band"), "ga"))
    return jax.shard_map(
        functools.partial(ace_of, mesh.shape["band"], mesh.shape["ga"]),
        mesh=mesh,
        in_specs=placed,
        out_specs=(P(("img", "band"), "ga"), P(("img", "band"), "ga")),
        check_vma=False,
    )
```

```python
import functools
import jax
import jax.numpy as jnp
from jax import lax
from jax.experimental import pallas as pl
from jax.experimental.pallas import tpu as pltpu
from jax.sharding import PartitionSpec as P

LANES = 128
SUB = 8
TILE = 128
PANEL = 32
GROUP = 2
CORES = 2
MESH = pl.DeviceIdType.MESH
F32 = jnp.float32
BF16 = jnp.bfloat16
VMEM = pl.BlockSpec(memory_space=pltpu.VMEM)


def row_of(value, index):
    return jnp.broadcast_to(value[index : index + 1, :], value.shape)


def column_of(value, index):
    return jnp.take_along_axis(value, jnp.full(value.shape, index, jnp.int32), axis=1)


def inverse_factor(rows, between=None):
    sub = lax.broadcasted_iota(jnp.int32, (SUB, LANES), 0)
    lane = lax.broadcasted_iota(jnp.int32, (SUB, LANES), 1)
    rows = list(rows)
    count = len(rows)
    per_panel = PANEL // SUB
    size = GROUP * SUB
    done = []
    for begin in range(0, count, GROUP):
        first = begin * SUB
        last = (begin // per_panel + 1) * per_panel
        inside = (lane >= first) & (lane < first + size)
        strips = rows[begin : begin + GROUP]
        columns = [[column_of(strip, first + k) for k in range(size)] for strip in strips]
        solved = [
            jnp.where(inside, jnp.where(lane - first == sub + s * SUB, 1.0, 0.0), strips[s])
            for s in range(GROUP)
        ]
        forward = list(solved)
        scale = [jnp.ones((SUB, LANES), F32)] * GROUP
        diagonal = [jnp.ones((SUB, LANES), F32)] * GROUP
        for j in range(size):
            js, jj = divmod(j, SUB)
            value = row_of(columns[js][j], jj)
            pivot = 1.0 / value
            here = sub == jj
            scale[js] = jnp.where(here, pivot, scale[js])
            diagonal[js] = jnp.where(here, value, diagonal[js])
            factor = [columns[s][j] * pivot for s in range(GROUP)]
            factor[js] = jnp.where(here, 0.0, factor[js])
            for k in range(j + 1, size):
                row = row_of(columns[js][k], jj)
                for s in range(GROUP):
                    columns[s][k] = columns[s][k] - factor[s] * row
            row = row_of(forward[js], jj)
            if jj < SUB - 1:
                forward[js] = forward[js] - jnp.where(sub > jj, factor[js], 0.0) * row
            for s in range(js + 1, GROUP):
                forward[s] = forward[s] - factor[s] * row
            row = row_of(solved[js], jj)
            for s in range(GROUP):
                solved[s] = solved[s] - factor[s] * row
        for s in range(GROUP):
            kept = forward[s] * lax.rsqrt(diagonal[s])
            stop = first + (s + 1) * SUB
            if stop < last * SUB:
                kept = jnp.where((lane < stop) | (lane >= last * SUB), kept, 0.0)
            done.append(kept)
        after = begin + GROUP
        if after < last:
            solved_rows = [row_of(solved[s] * scale[s], jj) for s in range(GROUP) for jj in range(SUB)]
            for r in range(after, last):
                old = rows[r]
                total = jnp.where(inside, 0.0, old)
                terms = [column_of(old, first + j) * solved_rows[j] for j in range(size)]
                while len(terms) > 1:
                    terms = [terms[i] + terms[i + 1] for i in range(0, len(terms), 2)]
                rows[r] = total - terms[0]
        elif last < count:
            if between is not None and last == count - per_panel:
                between()
            start = last - per_panel
            upper = jnp.concatenate(done[start:last], axis=0)
            high, low = split(upper)
            product = lax.dot_general(
                jnp.concatenate([high, high, low], axis=0),
                jnp.concatenate([high, low, high], axis=0),
                (((0,), (0,)), ((), ())),
                preferred_element_type=F32,
            )
            gone = (lane >= start * SUB) & (lane < last * SUB)
            for r in range(last, count):
                rows[r] = jnp.where(gone, 0.0, rows[r]) - product[r * SUB : r * SUB + SUB, :]
    return [jnp.where(lane < (t + 1) * SUB, done[t], 0.0) for t in range(count)]


def split(value):
    high = value.astype(BF16)
    return high, (value - high.astype(F32)).astype(BF16)


def dot(left, right):
    return lax.dot_general(left, right, (((1,), (0,)), ((), ())), preferred_element_type=F32)


def dot_rows(left, right):
    return lax.dot_general(left, right, (((1,), (1,)), ((), ())), preferred_element_type=F32)


def dot_split(left, right):
    (lh, ll), (rh, rl) = left, right
    return dot(jnp.concatenate([lh, lh, ll], axis=1), jnp.concatenate([rh, rl, rh], axis=0))


def remote(src, dst, send, recv, band, ga):
    return pltpu.make_async_remote_copy(
        src_ref=src,
        dst_ref=dst,
        send_sem=send,
        recv_sem=recv,
        device_id={"band": band, "ga": ga},
        device_id_type=MESH,
    )


def meet(devices):
    barrier = pltpu.get_barrier_semaphore()
    for band, ga in devices:
        pl.semaphore_signal(barrier, inc=1, device_id={"band": band, "ga": ga}, device_id_type=MESH)
    pl.semaphore_wait(barrier, len(devices))


def aligned(start, step, size):
    return pl.ds(pl.multiple_of(start, step), size)


def ring(position, count):
    return [(position + d) % count for d in range(1, count)]


def all_reduce(count, place, part, half_in, half, first_in, own, second_in, out, send, recv):
    core, here, there, along_first, along_second, pair = place
    piece = part.shape[0] // (CORES * count)
    size = piece * count
    pair_at, first_at, second_at, spread_at, give_at = 0, 1, count, 2 * count - 1, 3 * count - 2
    steps = range(1, count)

    def piece_at(q):
        return aligned((core * count + q) * piece, 16, piece)

    def copy_to(src, dst, sem, device):
        copy = remote(src, dst, send.at[sem], recv.at[sem], *device)
        copy.start()
        return copy

    swap = copy_to(part.at[aligned((1 - core) * size, 16, size), :], half_in, pair_at, pair)
    yield
    swap.wait()
    copies = []
    for d in range(1, count + 1):
        q = (here + d) % count
        theirs = half_in[aligned(q * piece, 16, piece), :].astype(F32)
        summed = part[piece_at(q), :].astype(F32) + theirs
        if d < count:
            half[d - 1] = summed.astype(BF16)
            copies.append(copy_to(half.at[d - 1], first_in.at[d - 1], first_at + d - 1, along_first(q)))
    yield
    for d, copy in enumerate(copies):
        copy.wait()
        summed = summed + first_in[d].astype(F32)
    own[...] = summed.astype(BF16)
    copies = []
    for d in steps:
        device = along_second((there + d) % count)
        copies.append(copy_to(own, second_in.at[there], second_at + d - 1, device))
    second_in[there] = own[...]
    yield
    for copy in copies:
        copy.wait()
    summed = second_in[0].astype(F32)
    for q in steps:
        summed = summed + second_in[q].astype(F32)
    out[piece_at(here), :] = summed.astype(BF16)
    copies, given = [], []

    def pass_on(slot, q):
        at = out.at[piece_at(q), :]
        given.append(copy_to(at, at, give_at + slot, pair))

    for d in steps:
        at = out.at[piece_at(here), :]
        copies.append(copy_to(at, at, spread_at + d - 1, along_first((here + d) % count)))
    pass_on(0, here)
    yield
    for d in steps:
        copies[d - 1].wait_recv()
        pass_on(d, (here - d + count) % count)
    yield
    for copy in copies:
        copy.wait_send()
    for copy in given:
        copy.wait()
    yield


def ace_kernel(
    count, groups, orbitals_ref, block_ref, kernel_ref, ace_out, exchange_out,
    orbitals, block, gains, bands, vectors, weighted, work, ace, exchange,
    *rest,
):
    head_refs, tail_refs, overlap_refs = rest[:7], rest[7:14], rest[14:21]
    (load, to_bands, from_bands, to_vectors, from_vectors, head_send, head_recv, tail_send, tail_recv,
     overlap_send, overlap_recv, to_ace, from_ace, to_block, from_block) = rest[21:]
    band, ga = lax.axis_index("band"), lax.axis_index("ga")
    line, core = ga // CORES, ga % CORES
    rows, cols = orbitals.shape[0], weighted.shape[1]
    block_rows = block.shape[0]
    total = orbitals.shape[1] * groups
    here = (1 - core) * band + core * line
    there = (1 - core) * line + core * band

    def along_first(q):
        return (1 - core) * q + core * band, CORES * ((1 - core) * line + core * q) + core

    def along_second(q):
        return (1 - core) * band + core * q, CORES * ((1 - core) * q + core * line) + core

    pair = (band, CORES * line + 1 - core)
    place = (core, here, there, along_first, along_second, pair)

    loads = [
        pltpu.make_async_copy(orbitals_ref, orbitals, load.at[0]),
        pltpu.make_async_copy(block_ref, block, load.at[1]),
        pltpu.make_async_copy(kernel_ref, gains, load.at[2]),
    ]
    for copy in loads:
        copy.start()
    meet(
        [along_first(q) for q in ring(here, count)]
        + [along_second(q) for q in ring(there, count)]
        + [pair]
    )
    for copy in loads:
        copy.wait()

    mine = aligned(band * cols, LANES, cols)
    band_rows = aligned(band * rows, 16, rows)
    vector_rows = aligned(band * block_rows, 16, block_rows)
    moved, moved_block = [], []
    for d, peer in enumerate(ring(band, count)):
        theirs = aligned(peer * cols, LANES, cols)
        moved.append(
            remote(orbitals.at[:, theirs], bands.at[band_rows, :], to_bands.at[d], from_bands.at[d], peer, ga)
        )
        moved_block.append(
            remote(block.at[:, theirs], vectors.at[vector_rows, :], to_vectors.at[d], from_vectors.at[d], peer, ga)
        )
    for copy in moved + moved_block:
        copy.start()
    bands[band_rows, :] = orbitals[:, mine]
    vectors[vector_rows, :] = block[:, mine]
    gain = gains[:, mine]
    for copy in moved:
        copy.wait()

    all_rows, all_vectors = bands.shape[0], vectors.shape[0]
    tiles, vector_tiles = all_rows // TILE, all_vectors // TILE
    head = {(0, j): j * TILE for j in range(tiles)}
    tail = [(i, j) for i in range(1, tiles) for j in range(i, tiles)]
    tail = {ij: n * TILE for n, ij in enumerate(tail)}
    flat = {(i, j): (i * vector_tiles + j) * TILE for i in range(tiles) for j in range(vector_tiles)}

    def clear_after(where, part):
        used = len(where) * TILE
        if used < part.shape[0]:
            part[used:, :] = jnp.zeros((part.shape[0] - used, LANES), BF16)

    def margin_rows(i, where, part):
        at, after = pl.ds(i * TILE, TILE), pl.ds(i * TILE, all_rows - i * TILE)
        sums = dot_rows(bands[at, :], weighted[after, :]) + dot_rows(weighted[at, :], bands[after, :])
        sums = (sums * (-0.5 / total)).astype(BF16)
        for j in range(i, tiles):
            part[pl.ds(where[i, j], TILE), :] = sums[:, (j - i) * TILE : (j - i + 1) * TILE]

    for i in range(tiles):
        at = pl.ds(i * TILE, TILE)
        weighted[at, :] = (-(bands[at, :].astype(F32) * gain)).astype(BF16)
    margin_rows(0, head, head_refs[0])
    clear_after(head, head_refs[0])
    head_steps = all_reduce(count, place, *head_refs, head_send, head_recv)
    next(head_steps)
    for i in range(1, tiles):
        margin_rows(i, tail, tail_refs[0])
    clear_after(tail, tail_refs[0])
    tail_steps = all_reduce(count, place, *tail_refs, tail_send, tail_recv)
    next(tail_steps)
    next(head_steps)
    for copy in moved_block:
        copy.wait()
    for i in range(tiles):
        sums = dot_rows(weighted[pl.ds(i * TILE, TILE), :], vectors[...])
        sums = (sums * (1.0 / total)).astype(BF16)
        for j in range(vector_tiles):
            overlap_refs[0][pl.ds(flat[i, j], TILE), :] = sums[:, j * TILE : (j + 1) * TILE]
    clear_after(flat, overlap_refs[0])
    overlap_steps = all_reduce(count, place, *overlap_refs, overlap_send, overlap_recv)
    next(overlap_steps)
    next(tail_steps)
    next(head_steps)
    next(overlap_steps)
    next(tail_steps)
    next(head_steps)
    next(overlap_steps)
    next(tail_steps)
    for i in range(tiles):
        at = pl.ds(i * TILE, TILE)
        work[at, pl.ds(all_rows, cols)] = weighted[at, :].astype(F32)
    next(head_steps)
    next(overlap_steps)
    next(head_steps)

    def unpack(where, out, column):
        for (i, j), row in where.items():
            work[pl.ds(i * TILE, TILE), pl.ds(column + j * TILE, TILE)] = out[pl.ds(row, TILE), :].astype(F32)

    def factored(value, between=None):
        strips = [value[SUB * t : SUB * (t + 1), :] for t in range(TILE // SUB)]
        return split(jnp.concatenate(inverse_factor(strips, between), axis=0))

    unpack(head, head_refs[-1], 0)
    inverse = factored(work[pl.ds(0, TILE), pl.ds(0, TILE)], lambda: next(tail_steps))
    next(tail_steps)
    next(overlap_steps)
    unpack(tail, tail_refs[-1], 0)
    edge = all_rows + cols
    segments, applied, early = [], None, None
    for k in range(tiles):
        top = k * TILE
        first = top + TILE
        ours = pl.ds(top, TILE)
        if k == 1:
            next(overlap_steps)
        ending = k == tiles - 1
        if not ending:
            at = pl.ds(first, TILE)
            ahead = split(dot_split(inverse, split(work[ours, at])))
            lower = split((ahead[0].astype(F32) + ahead[1].astype(F32)).T)
            value = work[at, at] - dot_split(lower, ahead)
            following = factored(value) if k < tiles - 4 else None
            lowers = [lower]
        else:
            lowers = []
        if k == 1:
            unpack(flat, overlap_refs[-1], edge)
            early_inverse, early_lowers, early_projector = early
            coupling = dot_split(early_inverse, split(work[pl.ds(0, TILE), pl.ds(edge, all_vectors)]))
            coupling_parts = split(coupling)
            for i in range(1, tiles):
                at = pl.ds(i * TILE, TILE), pl.ds(edge, all_vectors)
                work[at] = work[at] - dot_split(early_lowers[i - 1], coupling_parts)
            applied = dot_split(split(coupling.T), early_projector)
        start = min(first + TILE, all_rows)
        stop = edge if k == 0 else edge + all_vectors
        upper = dot_split(inverse, split(work[ours, pl.ds(start, stop - start)]))
        parts = split(upper)
        for i in range(k + 2, tiles):
            lowers.append(split(upper[:, i * TILE - start : (i + 1) * TILE - start].T))
        base = all_rows - start
        projector = tuple(part[:, base : base + cols] for part in parts)
        ace[ours, :] = projector[0]
        for p in range(count):
            low, high = max(top, p * rows), min(first, (p + 1) * rows)
            if low < high:
                target = pl.ds(low - p * rows, high - low)
                copy = remote(
                    ace.at[pl.ds(low, high - low), :], ace_out.at[target, mine],
                    to_ace.at[len(segments)], from_ace.at[band], p, ga,
                )
                segments.append((p, copy))
                pl.when(band != p)(copy.start)

                @pl.when(band == p)
                def _(low=low, high=high, target=target):
                    ace_out[target, mine] = ace[pl.ds(low, high - low), :]

        if not ending and following is None:
            following = factored(value)
        for i in range(k + 1, tiles):
            low = max(i * TILE, start)
            cut = tuple(part[:, low - start :] for part in parts)
            at = pl.ds(i * TILE, TILE), pl.ds(low, stop - low)
            work[at] = work[at] - dot_split(lowers[i - k - 1], cut)
        if k == 0:
            early = inverse, lowers, projector
        else:
            coupling = split(upper[:, base + cols :].T)
            applied = applied + dot_split(coupling, projector)
        if not ending:
            inverse = following
    exchange[...] = (-applied).astype(BF16)

    blocks = []
    for d, peer in enumerate(ring(band, count)):
        copy = remote(
            exchange.at[aligned(peer * block_rows, 16, block_rows), :], exchange_out.at[:, mine],
            to_block.at[d], from_block.at[d], peer, ga,
        )
        copy.start()
        blocks.append(copy)
    exchange_out[:, mine] = exchange[vector_rows, :]
    for p, copy in segments:
        pl.when(band != p)(copy.wait_send)
    for q in ring(band, count):
        remote(
            ace.at[pl.ds(0, rows), :], ace_out.at[:, aligned(q * cols, LANES, cols)],
            to_ace.at[0], from_ace.at[q], q, ga,
        ).wait_recv()
    for copy in blocks:
        copy.wait()


def ace_of(count, groups, orbitals, kernel, block_vectors):
    rows, coeffs = orbitals.shape
    block_rows = block_vectors.shape[0]
    bands, vectors, cols = rows * count, block_rows * count, coeffs // count
    tiles = bands // TILE
    dma = pltpu.SemaphoreType.DMA

    def reduced(used):
        pieces = CORES * count
        piece = pl.cdiv(pl.cdiv(used, pieces), 16) * 16
        return [
            pltpu.VMEM((pieces * piece, LANES), BF16),
            pltpu.VMEM((count * piece, LANES), BF16),
            pltpu.VMEM((count - 1, piece, LANES), BF16),
            pltpu.VMEM((count - 1, piece, LANES), BF16),
            pltpu.VMEM((piece, LANES), BF16),
            pltpu.VMEM((count, piece, LANES), BF16),
            pltpu.VMEM((pieces * piece, LANES), BF16),
        ]

    others = dma((count - 1,))
    reducing = dma((4 * count - 2,))
    anywhere = pl.BlockSpec(memory_space=pl.ANY)
    return pl.pallas_call(
        functools.partial(ace_kernel, count, groups),
        out_shape=(
            jax.ShapeDtypeStruct((rows, coeffs), BF16),
            jax.ShapeDtypeStruct((block_rows, coeffs), BF16),
        ),
        in_specs=[anywhere, anywhere, anywhere],
        out_specs=(VMEM, VMEM),
        scratch_shapes=[
            pltpu.VMEM((rows, coeffs), BF16),
            pltpu.VMEM((block_rows, coeffs), BF16),
            pltpu.VMEM((1, coeffs), F32),
            pltpu.VMEM((bands, cols), BF16),
            pltpu.VMEM((vectors, cols), BF16),
            pltpu.VMEM((bands, cols), BF16),
            pltpu.VMEM((bands, bands + cols + vectors), F32),
            pltpu.VMEM((bands, cols), BF16),
            pltpu.VMEM((vectors, cols), BF16),
            *reduced(tiles * TILE),
            *reduced(tiles * (tiles - 1) // 2 * TILE),
            *reduced(tiles * (vectors // TILE) * TILE),
            dma((3,)), others, others, others, others,
            reducing, reducing, reducing, reducing, reducing, reducing,
            dma((tiles + count,)), dma((count,)), others, others,
        ],
        compiler_params=pltpu.CompilerParams(
            collective_id=0, has_side_effects=True, vmem_limit_bytes=62 * 2**20
        ),
        name="ace",
    )(orbitals, block_vectors, kernel[None, :])


def solution(mesh):
    placed = (P(("img", "band"), "ga"), P("ga"), P(("img", "band"), "ga"))
    return jax.shard_map(
        functools.partial(ace_of, mesh.shape["band"], mesh.shape["ga"]),
        mesh=mesh,
        in_specs=placed,
        out_specs=(P(("img", "band"), "ga"), P(("img", "band"), "ga")),
        check_vma=False,
    )
```
